64 devices in a mesh: rep: 8 (over x, y, core), dp: 8 (over z).
Axes of the slice: x: 2, y: 2, z: 8, core: 2. Of those that a mesh axis runs over, the one named last changes fastest.
The devices are a block of a 4x4x8 slice.
Arguments:
- x: bfloat16 [64, 2048, 640], P(('rep', 'dp')), parts along dimension 0
- dy: bfloat16 [64, 2048, 640], P(('rep', 'dp')), parts along dimension 0
- w_gate: bfloat16 [2, 640, 1536], P(None, 'dp')
- w_up: bfloat16 [2, 640, 1536], P(None, 'dp')
- w_down: bfloat16 [2, 1536, 640], P(None, 'dp')
- m_w_gate: float32 [2, 640, 1536], P(None, 'dp')
- m_w_up: float32 [2, 640, 1536], P(None, 'dp')
- m_w_down: float32 [2, 1536, 640], P(None, 'dp')
- v_w_gate: float32 [2, 640, 1536], P(None, 'dp')
- v_w_up: float32 [2, 640, 1536], P(None, 'dp')
- v_w_down: float32 [2, 1536, 640], P(None, 'dp')
Outputs:
- output 1: bfloat16 [16, 640, 1536], P('rep', 'dp'), parts along dimension 0
- output 2: bfloat16 [16, 640, 1536], P('rep', 'dp'), parts along dimension 0
- output 3: bfloat16 [16, 1536, 640], P('rep', 'dp'), parts along dimension 0
- output 4: float32 [16, 640, 1536], P('rep', 'dp'), parts along dimension 0
- output 5: float32 [16, 640, 1536], P('rep', 'dp'), parts along dimension 0
- output 6: float32 [16, 1536, 640], P('rep', 'dp'), parts along dimension 0
- output 7: float32 [16, 640, 1536], P('rep', 'dp'), parts along dimension 0
- output 8: float32 [16, 640, 1536], P('rep', 'dp'), parts along dimension 0
- output 9: float32 [16, 1536, 640], P('rep', 'dp'), parts along dimension 0
There are 8 independent parts. The reference program is written for one: setup_inputs(seed, part) draws one part's arguments, and reference() takes and returns one part's arrays. A program takes and returns all parts, laid end to end along the dimension named above; an argument that names none is the same for every part.
All inputs are finite; a program needn't handle non-finite values.
Results may differ from the reference program's by a relative error of at most 0.022.
Values are sent between devices in bfloat16 or wider.
A program may use at most 768 MiB of HBM per device.

```python
import jax
import jax.numpy as jnp
from jax import lax

SEQUENCES = 8
TOKENS = 2048
D = 640
FF = 1536
LAYERS = 2
NAMES = ("w_gate", "w_up", "w_down")
SHAPES = {"w_gate": (LAYERS, D, FF), "w_up": (LAYERS, D, FF), "w_down": (LAYERS, FF, D)}


def bump(key, n, height):
    away = (jnp.arange(n, dtype=jnp.int32) - jax.random.randint(key, (), 0, n, jnp.int32)) % n
    return jnp.where(away < n // 8, height, 1.0)


def together(key, own, strength):
    shared = jax.random.normal(key, own.shape[1:], jnp.float32)
    return (own + strength * shared) * lax.rsqrt(1 + strength * strength)


def setup_inputs(seed: int = 0, part: int = 0) -> dict:
    kx, kdy, ka, kb, kz, kf, kh, kl, *keys = jax.random.split(jax.random.key(seed), 8 + 3 * len(NAMES))
    kx, kdy, ka, kb = (jax.random.fold_in(k, part) for k in (kx, kdy, ka, kb))
    kw, km, kv = (keys[i::3] for i in range(3))
    shape = (SEQUENCES, TOKENS, D)
    much_x, much_dy = jax.random.uniform(kz, (2,), jnp.float32, 0.0, 1.0)
    loud = 2.0 ** jax.random.uniform(jax.random.fold_in(kz, 1), (), jnp.float32, -1.0, 2.0)
    layers = 2.0 ** jax.random.uniform(kl, (LAYERS, 1, 1), jnp.float32, -1.0, 1.0)
    x = together(ka, jax.random.normal(kx, shape, jnp.float32), much_x) * bump(kf, D, 4.0)
    dy = together(kb, jax.random.normal(kdy, shape, jnp.float32), much_dy)
    drawn = {"x": x.astype(jnp.bfloat16), "dy": (loud * dy * (SEQUENCES * TOKENS) ** -0.5).astype(jnp.bfloat16)}
    for key, name in zip(kw, NAMES, strict=True):
        w = jax.random.normal(key, SHAPES[name], jnp.float32) * SHAPES[name][1] ** -0.5
        drawn[name] = (w * {"w_gate": 1.0, "w_up": bump(kh, FF, 4.0), "w_down": layers}[name]).astype(jnp.bfloat16)
    for key, name in zip(km, NAMES, strict=True):
        drawn[f"m_{name}"] = 0.1 * jax.random.normal(key, SHAPES[name], jnp.float32)
    for key, name in zip(kv, NAMES, strict=True):
        drawn[f"v_{name}"] = jax.random.uniform(key, SHAPES[name], jnp.float32, 0.005, 0.015)
    return drawn


def matmul(a, w):
    return jnp.dot(a, w, preferred_element_type=jnp.float32).astype(jnp.bfloat16)


def normed(h):
    wide = h.astype(jnp.float32)
    scale = lax.rsqrt(jnp.mean(wide**2, -1, keepdims=True) + 1e-6)
    return (wide * scale).astype(jnp.bfloat16)


def layer(h, w):
    a = normed(h)
    gate = jnp.dot(a, w["w_gate"], preferred_element_type=jnp.float32)
    up = jnp.dot(a, w["w_up"], preferred_element_type=jnp.float32)
    return h + matmul((jax.nn.silu(gate) * up).astype(jnp.bfloat16), w["w_down"])


def adamw(w, m, v, g):
    m = 0.9 * m + 0.1 * g
    v = 0.95 * v + 0.05 * g * g
    step = m * lax.rsqrt(v + 1e-8) + 0.1 * w
    return (w - 0.02 * step).astype(jnp.bfloat16), m, v


def clipped(gradients, sum_of_squares, count):
    factor = jnp.minimum(1.0, 0.5 * lax.rsqrt(sum_of_squares / count + 1e-30))
    return [g * factor for g in gradients]


def stack(weights, h):
    return lax.scan(lambda h, w: (layer(h, w), None), h, weights)[0]


def reference(x, dy, w_gate, w_up, w_down, m_w_gate, m_w_up, m_w_down, v_w_gate, v_w_up, v_w_down):
    weights = dict(zip(NAMES, (w_gate, w_up, w_down), strict=True))

    def take(so_far, sequence):
        h, by_y = sequence
        _, back = jax.vjp(lambda w: stack(w, h), weights)
        return jax.tree.map(lambda total, term: total + term.astype(jnp.float32), so_far, back(by_y)[0]), None

    none_yet = {name: jnp.zeros(w.shape, jnp.float32) for name, w in weights.items()}
    by_weights, _ = lax.scan(take, none_yet, (x, dy))
    gradients = [by_weights[name].astype(jnp.bfloat16).astype(jnp.float32) for name in NAMES]
    gradients = clipped(gradients, sum(jnp.sum(g * g) for g in gradients), sum(g.size for g in gradients))
    new = [
        adamw(w.astype(jnp.float32), m, v, g)
        for w, m, v, g in zip((w_gate, w_up, w_down), (m_w_gate, m_w_up, m_w_down), (v_w_gate, v_w_up, v_w_down), gradients, strict=True)
    ]
    return tuple(one[which] for which in range(3) for one in new)
```

```python
import functools

import jax
import jax.numpy as jnp
from jax import lax
from jax.experimental import pallas as pl
from jax.experimental.pallas import tpu as pltpu
from jax.sharding import PartitionSpec as P

BF, F32 = jnp.bfloat16, jnp.float32
TILE = 512
CH = 512


def mm(a, b):
    return jnp.dot(a, b, preferred_element_type=F32)


def mm_nt(a, b):
    return lax.dot_general(a, b, (((1,), (1,)), ((), ())), preferred_element_type=F32)


def scale_of(wide):
    return lax.rsqrt(jnp.mean(wide * wide, -1, keepdims=True) + 1e-6)


def kernel(n, x_hbm, dy_hbm, wg_in, wu_in, wd_in, og, ou, od, oss, *scratch):
    (wg, wu, wd, rg, ru, rd, mid, dg, du, at, dt, xb, yb, mine, theirs,
     aga_s, aga_r, agb_s, agb_r, agp_s, agp_r, rsa_s, rsa_r, rsb_s, rsb_r, all_s, all_r, loc) = scratch
    rep, z = lax.axis_index("rep"), lax.axis_index("dp")
    core = lax.rem(rep, 2)
    way = 1 - 2 * core
    ha = n // 2
    hb = n - 1 - ha
    tokens, d = xb.shape
    ff = mid.shape[1]

    def at_z(k):
        return lax.rem(z + way * k + n, n)

    near, far = at_z(1), at_z(-1)
    near_id, far_id, pair_id = (rep, near), (rep, far), (rep + way, z)

    barrier = pltpu.get_barrier_semaphore()
    for k in range(1, n):
        pl.semaphore_signal(barrier, inc=1, device_id=(rep, lax.rem(z + k, n)), device_id_type=pl.DeviceIdType.MESH)
    pl.semaphore_signal(barrier, inc=1, device_id=pair_id, device_id_type=pl.DeviceIdType.MESH)
    pl.semaphore_wait(barrier, n)

    full, shard, got, out = (wg, wu, wd), (wg_in, wu_in, wd_in), (rg, ru, rd), (og, ou, od)

    def half_of(i, ref, slot, block):
        rows, cols = shard[i].shape[1:]
        if i == 2:
            return ref.at[slot, pl.ds(pl.multiple_of(block * rows + core * (rows // 2), 16), rows // 2), :]
        return ref.at[slot, pl.ds(pl.multiple_of(block * rows, 16), rows), pl.ds(pl.multiple_of(core * (cols // 2), 128), cols // 2)]

    def rows_of(i, ref, slot, block):
        rows = shard[i].shape[1]
        return ref.at[slot, pl.ds(pl.multiple_of(block * rows, 16), rows), :]

    def remote(src, dst, send, recv, to):
        return pltpu.make_async_remote_copy(
            src_ref=src, dst_ref=dst, send_sem=send, recv_sem=recv, device_id=to, device_id_type=pl.DeviceIdType.MESH
        )

    def ag_a(m, s):
        i, l = m % 3, m // 3
        dst = half_of(i, full[i], l, at_z(-s))
        src = half_of(i, shard[i], l, 0) if s == 0 else dst
        return remote(src, dst, aga_s.at[m, s], aga_r.at[m, s], near_id)

    def ag_b(m, s):
        i, l = m % 3, m // 3
        dst = half_of(i, full[i], l, at_z(s))
        src = half_of(i, shard[i], l, 0) if s == 0 else dst
        return remote(src, dst, agb_s.at[m, s], agb_r.at[m, s], far_id)

    def ag_p(m, k):
        i, l = m % 3, m // 3
        block = at_z(-(k + 1)) if k < ha else at_z(k - ha + 1)
        ref = half_of(i, full[i], l, block)
        return remote(ref, ref, agp_s.at[m, k], agp_r.at[m, k], pair_id)

    def ag_tick(m, s):
        if s == 0:
            ag_a(m, 0).start()
            ag_b(m, 0).start()
            i, l = m % 3, m // 3
            rows = shard[i].shape[1]
            full[i][l, pl.ds(pl.multiple_of(z * rows, 16), rows), :] = shard[i][l]
            return
        if s <= ha:
            ag_a(m, s - 1).wait_recv()
            if s < ha:
                ag_a(m, s).start()
            ag_p(m, s - 1).start()
        if s <= hb:
            ag_b(m, s - 1).wait_recv()
            if s < hb:
                ag_b(m, s).start()
            ag_p(m, ha + s - 1).start()

    def ag_done(m):
        for k in range(n - 1):
            ag_p(m, k).wait_recv()

    def ag_drain(m):
        for s in range(ha):
            ag_a(m, s).wait_send()
        for s in range(hb):
            ag_b(m, s).wait_send()
        for k in range(n - 1):
            ag_p(m, k).wait_send()

    def slot_of(m):
        return 2 if m // 3 else 1

    def rs_a(m, s):
        i = m % 3
        src = rows_of(i, full[i], slot_of(m), at_z(ha - s))
        return remote(src, got[i].at[m // 3, s], rsa_s.at[m, s], rsa_r.at[m, s], near_id)

    def rs_b(m, s):
        i = m % 3
        src = rows_of(i, full[i], slot_of(m), at_z(-(hb - s)))
        return remote(src, got[i].at[m // 3, ha + s], rsb_s.at[m, s], rsb_r.at[m, s], far_id)

    def add_in(m, block, k):
        ref = rows_of(m % 3, full[m % 3], slot_of(m), block)
        ref[...] = (ref[...].astype(F32) + got[m % 3][m // 3, k].astype(F32)).astype(BF)

    def rs_tick(m, s):
        i = m % 3
        if s < ha:
            if s:
                rs_a(m, s - 1).wait_recv()
                add_in(m, at_z(ha - s), s - 1)
            rs_a(m, s).start()
        if 1 <= s <= hb:
            if s > 1:
                rs_b(m, s - 2).wait_recv()
                add_in(m, at_z(-(hb - s + 1)), ha + s - 2)
            rs_b(m, s - 1).start()
        if s == ha:
            rs_a(m, ha - 1).wait_recv()
            rs_b(m, hb - 1).wait_recv()
            own = rows_of(i, full[i], slot_of(m), z)[...].astype(F32)
            g = (own + got[i][m // 3, ha - 1].astype(F32) + got[i][m // 3, n - 2].astype(F32)).astype(BF)
            out[i][m // 3] = g
            wide = g.astype(F32)
            mine[...] += jnp.full(mine.shape, jnp.sum(wide * wide), F32)

    def rs_drain(m):
        for s in range(ha):
            rs_a(m, s).wait_send()
        for s in range(hb):
            rs_b(m, s).wait_send()

    def run(ticks):
        for kind, m, s in ticks:
            (ag_tick if kind == "a" else rs_tick)(m, s)

    def loop(steps, pieces, body, sched):
        def one(t, carry):
            for c in range(pieces):
                body(t, c)
                for (when, piece), ticks in sched.items():
                    if piece == c:
                        pl.when(t == when)(functools.partial(run, ticks))
            return carry

        lax.fori_loop(0, steps, one, 0)

    G0, U0, D0, G1, U1, D1 = range(6)
    steps, pieces = tokens // TILE, ff // CH
    mine[...] = jnp.zeros_like(mine)
    get_x = pltpu.make_async_copy(x_hbm, xb, loc.at[0])
    get_dy = pltpu.make_async_copy(dy_hbm, yb, loc.at[1])
    get_x.start()
    get_dy.start()

    a = lambda m, s: ("a", m, s)
    r = lambda m, s: ("r", m, s)
    run([a(G0, 0), a(U0, 0), a(G0, 1), a(U0, 1), a(G0, 2), a(U0, 2), a(D0, 0), a(G0, 3), a(U0, 3), a(G1, 0), a(G0, 4), a(U0, 4)])
    get_x.wait()
    run([a(D0, 1), a(G1, 1)])
    ag_done(G0)
    ag_done(U0)

    def rows_at(t):
        return pl.ds(pl.multiple_of(t * TILE, TILE), TILE)

    def cols(c):
        return pl.ds(c * CH, CH)

    def first(t, c):
        rows = rows_at(t)
        if c == 0:
            wide = xb[rows, :].astype(F32)
            a_tile = (wide * scale_of(wide)).astype(BF)
            du[rows, pl.ds(0, d)] = a_tile
        a_tile = du[rows, pl.ds(0, d)]
        gate, up = mm(a_tile, wg[0, :, cols(c)]), mm(a_tile, wu[0, :, cols(c)])
        mid[rows, cols(c)] = (gate * jax.nn.sigmoid(gate) * up).astype(BF)

    loop(steps, pieces, first, {
        (0, 1): [a(D0, 2), a(G1, 2)], (1, 0): [a(D0, 3), a(G1, 3), a(U1, 0)], (1, 2): [a(D1, 0), a(D0, 4), a(G1, 4)],
        (2, 2): [a(U1, 1), a(D1, 1)],
    })
    run([a(U1, 2), a(D1, 2)])
    ag_done(D0)

    def down(t, c):
        rows = rows_at(t)
        xb[rows, :] = (xb[rows, :].astype(F32) + mm(mid[rows, :], wd[0]).astype(BF).astype(F32)).astype(BF)

    loop(steps, 1, down, {(1, 0): [a(U1, 3), a(D1, 3)], (3, 0): [a(U1, 4), a(D1, 4)]})
    get_dy.wait()
    for m in (G1, U1, D1):
        ag_done(m)

    def hidden(l, h_ref, ct_ref):
        def body(t, c):
            rows = rows_at(t)
            if c == 0:
                wide = h_ref[rows, :].astype(F32)
                a_tile = (wide * scale_of(wide)).astype(BF)
                du[rows, pl.ds((pieces - 1) * CH, d - CH)] = a_tile[:, CH:]
                dg[rows, pl.ds((pieces - 1) * CH, CH)] = a_tile[:, :CH]
                at[:, rows] = a_tile.T
                dt[:, rows] = ct_ref[rows, :].T
            a_tile = jnp.concatenate(
                [dg[rows, pl.ds((pieces - 1) * CH, CH)], du[rows, pl.ds((pieces - 1) * CH, d - CH)]], axis=1
            )
            gate, up = mm(a_tile, wg[l, :, cols(c)]), mm(a_tile, wu[l, :, cols(c)])
            ct = mm_nt(ct_ref[rows, :], wd[l, cols(c), :]).astype(BF).astype(F32)
            s = jax.nn.sigmoid(gate)
            silu = gate * s
            mid[rows, cols(c)] = (silu * up).astype(BF)
            du[rows, cols(c)] = (ct * silu).astype(BF)
            by_silu = ct * up
            dg[rows, cols(c)] = (by_silu * (s * (1.0 + gate * (1.0 - s)))).astype(BF)

        return body

    loop(steps, pieces, hidden(1, xb, yb), {})
    for m in (G1, U1, D1):
        ag_drain(m)

    DC = ff // 4

    def term_down(slot):
        def body(c, _):
            cut = pl.ds(pl.multiple_of(c * DC, DC), DC)
            wd[slot, cut, :] = mm(dt[...], mid[:, cut]).astype(BF).T

        return body

    def term(ref, slot, by):
        def body(c, _):
            cut = pl.ds(pl.multiple_of(c * CH, CH), CH)
            ref[slot, :, cut] = mm(at[...], by[:, cut]).astype(BF)

        return body

    loop(ff // DC, 1, term_down(2), {})
    run([r(D1, 0)])
    loop(pieces, 1, term(wg, 2, dg), {(1, 0): [r(D1, 1)]})
    run([r(G1, 0)])
    loop(pieces, 1, term(wu, 2, du), {(0, 0): [r(D1, 2)], (1, 0): [r(G1, 1)]})
    run([r(U1, 0)])

    def by_input(t, c):
        rows = rows_at(t)
        wide = xb[rows, :].astype(F32)
        ct = mm_nt(dg[rows, :], wg[1]).astype(BF).astype(F32) + mm_nt(du[rows, :], wu[1]).astype(BF).astype(F32)
        ct = ct.astype(BF).astype(F32)
        scale = scale_of(wide)
        inner = jnp.sum(ct * wide, -1, keepdims=True) * (scale * scale * scale) * (1.0 / d)
        by_h = (ct * scale - wide * inner).astype(BF)
        xb[rows, :] = (yb[rows, :].astype(F32) + by_h.astype(F32)).astype(BF)

    loop(steps, 1, by_input, {(0, 0): [r(D1, 3), r(G1, 2)], (1, 0): [r(U1, 1)], (2, 0): [r(D1, 4), r(G1, 3)], (3, 0): [r(U1, 2)]})
    get_x = pltpu.make_async_copy(x_hbm, yb, loc.at[0])
    get_x.start()
    get_x.wait()

    loop(steps, pieces, hidden(0, yb, xb), {(0, 2): [r(G1, 4), r(U1, 3)], (2, 0): [r(U1, 4)]})
    loop(ff // DC, 1, term_down(1), {})
    run([r(D0, 0)])
    loop(pieces, 1, term(wg, 1, dg), {(1, 0): [r(D0, 1)]})
    run([r(G0, 0)])
    loop(pieces, 1, term(wu, 1, du), {(0, 0): [r(D0, 2)], (1, 0): [r(G0, 1)]})
    run([r(U0, 0)])
    run([r(D0, 3), r(G0, 2), r(U0, 1), r(D0, 4), r(G0, 3), r(U0, 2), r(G0, 4), r(U0, 3), r(U0, 4)])

    def tell(k):
        return remote(mine, theirs.at[z], all_s.at[k - 1], all_r.at[k - 1], (rep, lax.rem(z + k, n)))

    for k in range(1, n):
        tell(k).start()
    theirs[z] = mine[...]
    for m in (G0, U0, D0):
        ag_drain(m)
    for m in range(6):
        rs_drain(m)
    for k in range(1, n):
        tell(k).wait()
    oss[...] = jnp.sum(theirs[...], axis=0)


def adamw(w, m, v, g):
    m = 0.9 * m + 0.1 * g
    v = 0.95 * v + 0.05 * g * g
    step = m * lax.rsqrt(v + 1e-8) + 0.1 * w
    return (w - 0.02 * step).astype(BF), m, v


def clipped(gradients, sum_of_squares, count):
    factor = jnp.minimum(1.0, 0.5 * lax.rsqrt(sum_of_squares / count + 1e-30))
    return [g * factor for g in gradients]


def solution(mesh):
    n = mesh.shape["dp"]

    def step(x, dy, *arrays):
        weights, m, v = (arrays[i : i + 3] for i in (0, 3, 6))
        x, dy = x[0], dy[0]
        tokens, d = x.shape
        ff = weights[0].shape[2]
        ha, hb = n // 2, n - 1 - n // 2
        vmem = pl.BlockSpec(memory_space=pltpu.VMEM)
        anywhere = pl.BlockSpec(memory_space=pl.ANY)
        dma = pltpu.SemaphoreType.DMA
        flops = 17 * 2 * tokens * d * ff
        *gradients, squares = pl.pallas_call(
            functools.partial(kernel, n),
            out_shape=[jax.ShapeDtypeStruct(w.shape, BF) for w in weights] + [jax.ShapeDtypeStruct((8, 128), F32)],
            in_specs=[anywhere, anywhere, vmem, vmem, vmem],
            out_specs=[vmem] * 4,
            scratch_shapes=[
                pltpu.VMEM((3, d, ff), BF),
                pltpu.VMEM((3, d, ff), BF),
                pltpu.VMEM((3, ff, d), BF),
                *[pltpu.VMEM((2, n - 1, *w.shape[1:]), BF) for w in weights],
                *[pltpu.VMEM((tokens, ff), BF)] * 3,
                *[pltpu.VMEM((d, tokens), BF)] * 2,
                *[pltpu.VMEM((tokens, d), BF)] * 2,
                pltpu.VMEM((8, 128), F32),
                pltpu.VMEM((n, 8, 128), F32),
                dma((6, ha)), dma((6, ha)), dma((6, hb)), dma((6, hb)), dma((6, n - 1)), dma((6, n - 1)),
                dma((6, ha)), dma((6, ha)), dma((6, hb)), dma((6, hb)), dma((n - 1,)), dma((n - 1,)), dma((2,)),
            ],
            compiler_params=pltpu.CompilerParams(collective_id=0, has_side_effects=True, vmem_limit_bytes=67043328),
            cost_estimate=pl.CostEstimate(flops=flops, bytes_accessed=10 * tokens * d, transcendentals=0),
        )(x, dy, *weights)
        gradients = [g.astype(F32) for g in gradients]
        gradients = clipped(gradients, squares[0, 0], n * sum(g.size for g in gradients))
        new = [adamw(w.astype(F32), m, v, g) for w, m, v, g in zip(weights, m, v, gradients, strict=True)]
        return tuple(one[which] for which in range(3) for one in new)

    states, cut = P(("rep", "dp"), None, None), P(None, "dp", None)
    return jax.shard_map(
        step,
        mesh=mesh,
        in_specs=(states, states) + (cut,) * 9,
        out_specs=(P("rep", "dp", None),) * 9,
        check_vma=False,
    )
```

```python
import functools

import jax
import jax.numpy as jnp
from jax import lax
from jax.experimental import pallas as pl
from jax.experimental.pallas import tpu as pltpu
from jax.sharding import PartitionSpec as P

BF, F32 = jnp.bfloat16, jnp.float32
TILE = 512
CH = 512
LAG = 1.8


def mm(a, b):
    return jnp.dot(a, b, preferred_element_type=F32)


def mm_nt(a, b):
    return lax.dot_general(a, b, (((1,), (1,)), ((), ())), preferred_element_type=F32)


def scale_of(wide):
    return lax.rsqrt(jnp.mean(wide * wide, -1, keepdims=True) + 1e-6)


def plan(segments, hops, pieces):
    now, free, todo, agenda = 0.0, 0.0, [], {}

    def start(tick):
        nonlocal free
        l, p, s, _ = tick
        cost = (5.27 if p == 2 * pieces else 1.76) * (0.0 if s == hops else 0.5 if s == hops - 1 else 1.0)
        free = max(free, now) + cost
        tick[2:] = [s + 1, free + LAG]
        return (l, p, s)

    for l, kind, steps, each in segments:
        for step in range(steps):
            now += each
            if kind[:4] == "term":
                todo.append([l, step * pieces + int(kind[4:]), 0, now])
            if kind == "down" and step == steps - 1:
                todo.append([l, 2 * pieces, 0, now])
            due = sorted((t for t in todo if t[3] <= now), key=lambda t: t[3])
            if due:
                agenda[l, kind, step] = [start(t) for t in due]
            todo = [t for t in todo if t[2] <= hops]
    after = []
    while todo:
        tick = min(todo, key=lambda t: t[3])
        now = max(now, tick[3])
        after.append(start(tick))
        todo = [t for t in todo if t[2] <= hops]
    return agenda | {"after": after}


def kernel(n, x_hbm, dy_hbm, wg_in, wu_in, wd_in, og, ou, od, oss, *scratch):
    (wg, wu, wd, rg, ru, rd, mid, dg, du, at, dt, xb, yb, mine, theirs,
     agz_s, agz_r, agy_s, agy_r, agp_s, agp_r, rsa_s, rsa_r, rsb_s, rsb_r, all_s, all_r, loc) = scratch
    rep, z = lax.axis_index("rep"), lax.axis_index("dp")
    core = lax.rem(rep, 2)
    way = 1 - 2 * core
    chip = lax.rem(rep // 2, 2)
    ha = n // 2
    hb = n - 1 - ha
    tokens, d = xb.shape
    ff = mid.shape[1]

    def at_z(k):
        return lax.rem(z + way * k + n, n)

    near, far = at_z(1), at_z(-1)
    near_id, far_id, pair_id, side_id = (rep, near), (rep, far), (rep + way, z), (rep + 2 - 4 * chip, z)

    barrier = pltpu.get_barrier_semaphore()
    for k in range(1, n):
        pl.semaphore_signal(barrier, inc=1, device_id=(rep, lax.rem(z + k, n)), device_id_type=pl.DeviceIdType.MESH)
    for other in (pair_id, side_id):
        pl.semaphore_signal(barrier, inc=1, device_id=other, device_id_type=pl.DeviceIdType.MESH)
    with jax.named_scope("entry"):
        pl.semaphore_wait(barrier, n + 1)

    steps, pieces = tokens // TILE, ff // CH
    full, shard, got, out = (wg, wu, wd), (wg_in, wu_in, wd_in), (rg, ru, rd), (og, ou, od)

    def cut_of(i, ref, slot, block, first, count):
        rows, cols = shard[i].shape[1:]
        if i == 2:
            third = rows // 6
            return ref.at[slot, pl.ds(pl.multiple_of(block * rows + core * (3 * third) + first * third, 16), count * third), :]
        third = cols // 6
        return ref.at[
            slot, pl.ds(pl.multiple_of(block * rows, 16), rows), pl.ds(pl.multiple_of(core * (3 * third) + first * third, 128), count * third)
        ]

    def remote(src, dst, send, recv, to):
        return pltpu.make_async_remote_copy(
            src_ref=src, dst_ref=dst, send_sem=send, recv_sem=recv, device_id=to, device_id_type=pl.DeviceIdType.MESH
        )

    def block_of(hop):
        return at_z(-(hop + 1)) if hop < ha else at_z(hop - ha + 1)

    def ag_ring(m, hop):
        i, l = m % 3, m // 3
        s = hop if hop < ha else hop - ha
        block = at_z(-s) if hop < ha else at_z(s)
        dst = cut_of(i, full[i], l, block, chip, 2)
        src = cut_of(i, shard[i], l, 0, chip, 2) if s == 0 else dst
        return remote(src, dst, agz_s.at[m, hop], agz_r.at[m, hop], near_id if hop < ha else far_id)

    def ag_side(m, hop):
        ref = cut_of(m % 3, full[m % 3], m // 3, block_of(hop), 2 * chip, 1)
        return remote(ref, ref, agy_s.at[m, hop], agy_r.at[m, hop], side_id)

    def ag_pair(m, hop, from_side):
        first, count = (2 - 2 * chip, 1) if from_side else (chip, 2)
        ref = cut_of(m % 3, full[m % 3], m // 3, block_of(hop), first, count)
        k = from_side * (n - 1) + hop
        return remote(ref, ref, agp_s.at[m, k], agp_r.at[m, k], pair_id)

    def ag_tick(m, s):
        if s == 0:
            ag_ring(m, 0).start()
            ag_ring(m, ha).start()
            i, l = m % 3, m // 3
            rows = shard[i].shape[1]
            full[i][l, pl.ds(pl.multiple_of(z * rows, 16), rows), :] = shard[i][l]
        for base, hops in ((0, ha), (ha, hb)):
            if 1 <= s <= hops:
                hop = base + s - 1
                ag_ring(m, hop).wait_recv()
                if s < hops:
                    ag_ring(m, hop + 1).start()
                ag_side(m, hop).start()
                ag_pair(m, hop, False).start()
        for base, hops in ((0, ha), (ha, hb)):
            if 2 <= s <= hops + 1:
                hop = base + s - 2
                ag_side(m, hop).wait_recv()
                ag_pair(m, hop, True).start()

    def ag_done(m):
        with jax.named_scope(f"done{m}"):
            for hop in range(n - 1):
                ag_pair(m, hop, False).wait_recv()
                ag_pair(m, hop, True).wait_recv()

    def ag_drain(m):
        for hop in range(n - 1):
            ag_ring(m, hop).wait_send()
            ag_side(m, hop).wait_send()
            ag_pair(m, hop, False).wait_send()
            ag_pair(m, hop, True).wait_send()

    def parts_of(l, p):
        i = p // pieces
        return i, pl.ds(p % pieces * CH, CH) if i < 2 else slice(None), l * (2 * pieces + 1) + p

    def rs_ref(i, l, block, cut):
        rows = shard[i].shape[1]
        return full[i].at[1 + l, pl.ds(pl.multiple_of(block * rows, 16), rows), cut]

    def rs_a(l, p, s):
        i, cut, sem = parts_of(l, p)
        return remote(rs_ref(i, l, at_z(ha - s), cut), got[i].at[l, s, :, cut], rsa_s.at[sem, s], rsa_r.at[sem, s], near_id)

    def rs_b(l, p, s):
        i, cut, sem = parts_of(l, p)
        return remote(rs_ref(i, l, at_z(-(hb - s)), cut), got[i].at[l, ha + s, :, cut], rsb_s.at[sem, s], rsb_r.at[sem, s], far_id)

    def rs_tick(l, p, s):
        i, cut, _ = parts_of(l, p)
        for copy, hops, base, sense in ((rs_a, ha, 0, 1), (rs_b, hb, ha, -1)):
            if s and s <= hops:
                copy(l, p, s - 1).wait_recv()
            if s < hops:
                if s:
                    ref = rs_ref(i, l, at_z(sense * (hops - s)), cut)
                    ref[...] = (ref[...].astype(F32) + got[i][l, base + s - 1, :, cut].astype(F32)).astype(BF)
                copy(l, p, s).start()
        if s == ha:
            own = rs_ref(i, l, z, cut)[...].astype(F32)
            g = (own + got[i][l, ha - 1, :, cut].astype(F32) + got[i][l, n - 2, :, cut].astype(F32)).astype(BF)
            out[i][l, :, cut] = g
            wide = g.astype(F32)
            mine[...] += jnp.full(mine.shape, jnp.sum(wide * wide), F32)

    def rs_drain(l, p):
        for s in range(ha):
            rs_a(l, p, s).wait_send()
        for s in range(hb):
            rs_b(l, p, s).wait_send()

    def run(ticks):
        for m, *s in ticks:
            with jax.named_scope(f"t{m}{s}"):
                rs_tick(m, *s) if len(s) == 2 else ag_tick(m, *s)

    def loop(steps, pieces, body, sched, name="loop"):
        def one(t, carry):
            for c in range(pieces):
                body(t, c)
                for (when, piece), ticks in sched.items():
                    if piece == c:
                        pl.when(t == when)(functools.partial(run, ticks))
            return carry

        with jax.named_scope(name):
            lax.fori_loop(0, steps, one, 0)

    G0, U0, D0, G1, U1, D1 = range(6)
    mine[...] = jnp.zeros_like(mine)
    get_x = pltpu.make_async_copy(x_hbm, xb, loc.at[0])
    get_dy = pltpu.make_async_copy(dy_hbm, yb, loc.at[1])
    get_x.start()
    get_dy.start()

    a = lambda m, s: (m, s)
    run([a(m, s) for s in range(ha) for m in (G0, U0, D0)])
    run([a(G1, 0), a(G0, 4), a(U1, 0), a(U0, 4), a(D1, 0), a(D0, 4), a(G0, 5), a(U0, 5), a(G1, 1), a(D0, 5)])
    get_x.wait()
    for m in (G0, U0, D0):
        ag_done(m)

    def rows_at(t):
        return pl.ds(pl.multiple_of(t * TILE, TILE), TILE)

    def cols(c):
        return pl.ds(c * CH, CH)

    def first(t, c):
        rows = rows_at(t)
        if c == 0:
            wide = xb[rows, :].astype(F32)
            a_tile = (wide * scale_of(wide)).astype(BF)
            du[rows, pl.ds(0, d)] = a_tile
        a_tile = du[rows, pl.ds(0, d)]
        gate, up = mm(a_tile, wg[0, :, cols(c)]), mm(a_tile, wu[0, :, cols(c)])
        mid[rows, cols(c)] = (gate * jax.nn.sigmoid(gate) * up).astype(BF)

    loop(steps, pieces, first, {
        (0, 0): [a(U1, 1)], (0, 2): [a(D1, 1)], (1, 0): [a(G1, 2)], (1, 2): [a(U1, 2)], (2, 0): [a(D1, 2)], (2, 2): [a(G1, 3)],
        (3, 0): [a(U1, 3)], (3, 2): [a(D1, 3)],
    }, "first")

    def down(t, c):
        rows = rows_at(t)
        xb[rows, :] = (xb[rows, :].astype(F32) + mm(mid[rows, :], wd[0]).astype(BF).astype(F32)).astype(BF)

    loop(steps, 1, down, {(0, 0): [a(G1, 4)], (1, 0): [a(U1, 4)], (2, 0): [a(D1, 4), a(G1, 5)], (3, 0): [a(U1, 5), a(D1, 5)]}, "down0")
    get_dy.wait()
    for m in (G1, U1, D1):
        ag_done(m)

    DC = ff // 4
    segments = []
    for l in (1, 0):
        segments += [(l, "prep", steps, 0.6)]
        for p in range(pieces):
            segments += [(l, f"hidden{p}", steps, 1.6), (l, f"term{p}", 2, 1.5)]
        segments += [(l, "down", ff // DC, 1.6)]
        if l:
            segments += [(l, "input", steps, 3.1)]
    agenda = plan(segments, ha, pieces)

    def hidden(l, h_ref, ct_ref):
        last = (pieces - 1) * CH

        def prep(t, _):
            rows = rows_at(t)
            wide = h_ref[rows, :].astype(F32)
            a_tile = (wide * scale_of(wide)).astype(BF)
            dg[rows, pl.ds(last, CH)] = a_tile[:, :CH]
            du[rows, pl.ds(last, d - CH)] = a_tile[:, CH:]
            at[:, rows] = a_tile.T
            dt[:, rows] = ct_ref[rows, :].T

        def piece(t, cut):
            rows = rows_at(t)
            a_tile = jnp.concatenate([dg[rows, pl.ds(last, CH)], du[rows, pl.ds(last, d - CH)]], axis=1)
            gate, up = mm(a_tile, wg[l, :, cut]), mm(a_tile, wu[l, :, cut])
            ct = mm_nt(ct_ref[rows, :], wd[l, cut, :]).astype(BF).astype(F32)
            s = jax.nn.sigmoid(gate)
            silu = gate * s
            mid[rows, cut] = (silu * up).astype(BF)
            du[rows, cut] = (ct * silu).astype(BF)
            dg[rows, cut] = (ct * up * (s * (1.0 + gate * (1.0 - s)))).astype(BF)

        loop(steps, 1, prep, {(t, 0): agenda[l, "prep", t] for t in range(steps) if (l, "prep", t) in agenda}, "prep")

        def one_piece(p, carry):
            cut = pl.ds(pl.multiple_of(p * CH, CH), CH)

            def tile(t, carry):
                piece(t, cut)
                for q in range(pieces):
                    for when in range(steps):
                        if (l, f"hidden{q}", when) in agenda:
                            pl.when((p == q) & (t == when))(functools.partial(run, agenda[l, f"hidden{q}", when]))
                return carry

            with jax.named_scope("hidden"):
                lax.fori_loop(0, steps, tile, 0)
            with jax.named_scope("term"):
                for which, (ref, by) in enumerate(((wg, dg), (wu, du))):
                    ref[1 + l, :, cut] = mm(at[...], by[:, cut]).astype(BF)
                    for q in range(pieces):
                        if (l, f"term{q}", which) in agenda:
                            pl.when(p == q)(functools.partial(run, agenda[l, f"term{q}", which]))
            return carry

        lax.fori_loop(0, pieces, one_piece, 0)

        def term_down(c, _):
            cut = pl.ds(pl.multiple_of(c * DC, DC), DC)
            wd[1 + l, cut, :] = mm(dt[...], mid[:, cut]).astype(BF).T

        loop(ff // DC, 1, term_down, {(t, 0): agenda[l, "down", t] for t in range(ff // DC) if (l, "down", t) in agenda}, "down")

    hidden(1, xb, yb)

    def by_input(t, c):
        rows = rows_at(t)
        wide = xb[rows, :].astype(F32)
        ct = mm_nt(dg[rows, :], wg[1]).astype(BF).astype(F32) + mm_nt(du[rows, :], wu[1]).astype(BF).astype(F32)
        ct = ct.astype(BF).astype(F32)
        scale = scale_of(wide)
        inner = jnp.sum(ct * wide, -1, keepdims=True) * (scale * scale * scale) * (1.0 / d)
        by_h = (ct * scale - wide * inner).astype(BF)
        xb[rows, :] = (yb[rows, :].astype(F32) + by_h.astype(F32)).astype(BF)

    loop(steps, 1, by_input, {(t, 0): agenda[1, "input", t] for t in range(steps) if (1, "input", t) in agenda}, "input")
    get_x = pltpu.make_async_copy(x_hbm, yb, loc.at[0])
    get_x.start()
    for m in (G1, U1, D1):
        ag_drain(m)
    get_x.wait()
    hidden(0, yb, xb)
    run(agenda["after"])

    def tell(k):
        return remote(mine, theirs.at[z], all_s.at[k - 1], all_r.at[k - 1], (rep, lax.rem(z + k, n)))

    for k in range(1, n):
        tell(k).start()
    theirs[z] = mine[...]
    with jax.named_scope("drain"):
      for m in (G0, U0, D0):
        ag_drain(m)
      for l in (0, 1):
          for p in range(2 * pieces + 1):
            rs_drain(l, p)
    with jax.named_scope("tell"):
        for k in range(1, n):
            tell(k).wait()
    oss[...] = jnp.sum(theirs[...], axis=0)


def adamw(w, m, v, g):
    m = 0.9 * m + 0.1 * g
    v = 0.95 * v + 0.05 * g * g
    step = m * lax.rsqrt(v + 1e-8) + 0.1 * w
    return (w - 0.02 * step).astype(BF), m, v


def clipped(gradients, sum_of_squares, count):
    factor = jnp.minimum(1.0, 0.5 * lax.rsqrt(sum_of_squares / count + 1e-30))
    return [g * factor for g in gradients]


def solution(mesh):
    n = mesh.shape["dp"]

    def step(x, dy, *arrays):
        weights, m, v = (arrays[i : i + 3] for i in (0, 3, 6))
        x, dy = x[0], dy[0]
        tokens, d = x.shape
        ff = weights[0].shape[2]
        ha, hb = n // 2, n - 1 - n // 2
        vmem = pl.BlockSpec(memory_space=pltpu.VMEM)
        anywhere = pl.BlockSpec(memory_space=pl.ANY)
        dma = pltpu.SemaphoreType.DMA
        flops = 17 * 2 * tokens * d * ff
        *gradients, squares = pl.pallas_call(
            functools.partial(kernel, n),
            out_shape=[jax.ShapeDtypeStruct(w.shape, BF) for w in weights] + [jax.ShapeDtypeStruct((8, 128), F32)],
            in_specs=[anywhere, anywhere, vmem, vmem, vmem],
            out_specs=[vmem] * 4,
            scratch_shapes=[
                pltpu.VMEM((3, d, ff), BF),
                pltpu.VMEM((3, d, ff), BF),
                pltpu.VMEM((3, ff, d), BF),
                *[pltpu.VMEM((2, n - 1, *w.shape[1:]), BF) for w in weights],
                *[pltpu.VMEM((tokens, ff), BF)] * 3,
                *[pltpu.VMEM((d, tokens), BF)] * 2,
                *[pltpu.VMEM((tokens, d), BF)] * 2,
                pltpu.VMEM((8, 128), F32),
                pltpu.VMEM((n, 8, 128), F32),
                dma((6, n - 1)), dma((6, n - 1)), dma((6, n - 1)), dma((6, n - 1)), dma((6, 2 * n - 2)), dma((6, 2 * n - 2)),
                dma((2 * (2 * (ff // CH) + 1), ha)), dma((2 * (2 * (ff // CH) + 1), ha)), dma((2 * (2 * (ff // CH) + 1), hb)), dma((2 * (2 * (ff // CH) + 1), hb)), dma((n - 1,)), dma((n - 1,)), dma((2,)),
            ],
            compiler_params=pltpu.CompilerParams(collective_id=0, has_side_effects=True, vmem_limit_bytes=67043328),
            cost_estimate=pl.CostEstimate(flops=flops, bytes_accessed=10 * tokens * d, transcendentals=0),
        )(x, dy, *weights)
        gradients = [g.astype(F32) for g in gradients]
        gradients = clipped(gradients, squares[0, 0], n * sum(g.size for g in gradients))
        new = [adamw(w.astype(F32), m, v, g) for w, m, v, g in zip(weights, m, v, gradients, strict=True)]
        return tuple(one[which] for which in range(3) for one in new)

    states, cut = P(("rep", "dp"), None, None), P(None, "dp", None)
    return jax.shard_map(
        step,
        mesh=mesh,
        in_specs=(states, states) + (cut,) * 9,
        out_specs=(P("rep", "dp", None),) * 9,
        check_vma=False,
    )
```

```python
import functools

import jax
import jax.numpy as jnp
from jax import lax
from jax.experimental import pallas as pl
from jax.experimental.pallas import tpu as pltpu
from jax.sharding import PartitionSpec as P

BF, F32 = jnp.bfloat16, jnp.float32
TILE = 512
CH = 512
LAG = 2
STEP = 0.2


def mm(a, b):
    return jnp.dot(a, b, preferred_element_type=F32)


def mm_nt(a, b):
    return lax.dot_general(a, b, (((1,), (1,)), ((), ())), preferred_element_type=F32)


def scale_of(wide):
    return lax.rsqrt(jnp.mean(wide * wide, -1, keepdims=True) + 1e-6)


def plan(segments, hops, pieces):
    now, free, todo, agenda = 0.0, 0.0, [], {}

    def start(tick):
        nonlocal free
        l, p, s, _ = tick
        cost = (2.63 if p >= 2 * pieces else 1.76) * (0.0 if s == hops else 0.5 if s == hops - 1 else 1.0)
        free = max(free, now) + cost
        tick[2:] = [s + 1, free + LAG]
        return (l, p, s)

    for l, kind, steps, each in segments:
        for step in range(steps):
            now += each
            if kind[:4] == "term":
                todo.append([l, step * pieces + int(kind[4:]), 0, now])
            if kind == "down" and step == steps - 1:
                todo += [[l, 2 * pieces, 0, now], [l, 2 * pieces + 1, 0, now]]
            due = sorted((t for t in todo if t[3] <= now), key=lambda t: (t[2], -t[1]))
            if due:
                agenda[l, kind, step] = [start(t) for t in due]
            todo = [t for t in todo if t[2] <= hops]
    after = []
    while todo:
        now = max(now, min(t[3] for t in todo))
        tick = min((t for t in todo if t[3] <= now), key=lambda t: (t[2], -t[1]))
        after.append(start(tick))
        now += STEP
        todo = [t for t in todo if t[2] <= hops]
    return agenda | {"after": after}


def kernel(n, x_hbm, dy_hbm, wg_in, wu_in, wd_in, og, ou, od, factor, *scratch):
    (wg, wu, wd, rg, ru, rd, mid, dg, du, at, dt, xb, yb, mine, theirs,
     agz_s, agz_r, agy_s, agy_r, agp_s, agp_r, rsa_s, rsa_r, rsb_s, rsb_r, all_s, all_r, loc) = scratch
    rep, z = lax.axis_index("rep"), lax.axis_index("dp")
    core = lax.rem(rep, 2)
    way = 1 - 2 * core
    chip = lax.rem(rep // 2, 2)
    ha = n // 2
    hb = n - 1 - ha
    tokens, d = xb.shape
    ff = mid.shape[1]

    def at_z(k):
        return lax.rem(z + way * k + n, n)

    near, far = at_z(1), at_z(-1)
    near_id, far_id, pair_id, side_id = (rep, near), (rep, far), (rep + way, z), (rep + 2 - 4 * chip, z)

    barrier = pltpu.get_barrier_semaphore()
    for k in range(1, n):
        pl.semaphore_signal(barrier, inc=1, device_id=(rep, lax.rem(z + k, n)), device_id_type=pl.DeviceIdType.MESH)
    for other in (pair_id, side_id):
        pl.semaphore_signal(barrier, inc=1, device_id=other, device_id_type=pl.DeviceIdType.MESH)
    with jax.named_scope("entry"):
        pl.semaphore_wait(barrier, n + 1)

    steps, pieces = tokens // TILE, ff // CH
    full, shard, got, out = (wg, wu, wd), (wg_in, wu_in, wd_in), (rg, ru, rd), (og, ou, od)

    def cut_of(i, ref, slot, block, first, count):
        rows, cols = shard[i].shape[1:]
        if i == 2:
            third = rows // 6
            return ref.at[slot, pl.ds(pl.multiple_of(block * rows + core * (3 * third) + first * third, 16), count * third), :]
        third = cols // 6
        return ref.at[
            slot, pl.ds(pl.multiple_of(block * rows, 16), rows), pl.ds(pl.multiple_of(core * (3 * third) + first * third, 128), count * third)
        ]

    def remote(src, dst, send, recv, to):
        return pltpu.make_async_remote_copy(
            src_ref=src, dst_ref=dst, send_sem=send, recv_sem=recv, device_id=to, device_id_type=pl.DeviceIdType.MESH
        )

    def block_of(hop):
        return at_z(-(hop + 1)) if hop < ha else at_z(hop - ha + 1)

    def ag_ring(m, hop):
        i, l = m % 3, m // 3
        s = hop if hop < ha else hop - ha
        block = at_z(-s) if hop < ha else at_z(s)
        dst = cut_of(i, full[i], l, block, chip, 2)
        src = cut_of(i, shard[i], l, 0, chip, 2) if s == 0 else dst
        return remote(src, dst, agz_s.at[m, hop], agz_r.at[m, hop], near_id if hop < ha else far_id)

    def ag_side(m, hop):
        ref = cut_of(m % 3, full[m % 3], m // 3, block_of(hop), 2 * chip, 1)
        return remote(ref, ref, agy_s.at[m, hop], agy_r.at[m, hop], side_id)

    def ag_pair(m, hop, from_side):
        first, count = (2 - 2 * chip, 1) if from_side else (chip, 2)
        ref = cut_of(m % 3, full[m % 3], m // 3, block_of(hop), first, count)
        k = from_side * (n - 1) + hop
        return remote(ref, ref, agp_s.at[m, k], agp_r.at[m, k], pair_id)

    def ag_tick(m, s):
        if s == 0:
            ag_ring(m, 0).start()
            ag_ring(m, ha).start()
            i, l = m % 3, m // 3
            rows = shard[i].shape[1]
            full[i][l, pl.ds(pl.multiple_of(z * rows, 16), rows), :] = shard[i][l]
        for base, hops in ((0, ha), (ha, hb)):
            if 1 <= s <= hops:
                hop = base + s - 1
                ag_ring(m, hop).wait_recv()
                if s < hops:
                    ag_ring(m, hop + 1).start()
                ag_side(m, hop).start()
                ag_pair(m, hop, False).start()
        for base, hops in ((0, ha), (ha, hb)):
            if 2 <= s <= hops + 1:
                hop = base + s - 2
                ag_side(m, hop).wait_recv()
                ag_pair(m, hop, True).start()

    def ag_done(m):
        with jax.named_scope(f"done{m}"):
            for hop in range(n - 1):
                ag_pair(m, hop, False).wait_recv()
                ag_pair(m, hop, True).wait_recv()

    def ag_drain(m):
        for hop in range(n - 1):
            ag_ring(m, hop).wait_send()
            ag_side(m, hop).wait_send()
            ag_pair(m, hop, False).wait_send()
            ag_pair(m, hop, True).wait_send()

    def parts_of(l, p):
        sem = l * (2 * pieces + 2) + p
        if p < 2 * pieces:
            return p // pieces, pl.ds(0, wg_in.shape[1]), pl.ds(p % pieces * CH, CH), sem
        half = wd_in.shape[1] // 2
        return 2, pl.ds((p - 2 * pieces) * half, half), slice(None), sem

    def rs_ref(i, l, block, part, cut):
        return full[i].at[1 + l, pl.ds(pl.multiple_of(block * shard[i].shape[1] + part.start, 16), part.size), cut]

    def rs_a(l, p, s):
        i, part, cut, sem = parts_of(l, p)
        return remote(rs_ref(i, l, at_z(ha - s), part, cut), got[i].at[l, s, part, cut], rsa_s.at[sem, s], rsa_r.at[sem, s], near_id)

    def rs_b(l, p, s):
        i, part, cut, sem = parts_of(l, p)
        return remote(
            rs_ref(i, l, at_z(-(hb - s)), part, cut), got[i].at[l, ha + s, part, cut], rsb_s.at[sem, s], rsb_r.at[sem, s], far_id
        )

    def rs_tick(l, p, s):
        i, part, cut, _ = parts_of(l, p)
        for copy, hops, base, sense in ((rs_a, ha, 0, 1), (rs_b, hb, ha, -1)):
            if s and s <= hops:
                copy(l, p, s - 1).wait_recv()
            if s < hops:
                if s:
                    ref = rs_ref(i, l, at_z(sense * (hops - s)), part, cut)
                    ref[...] = (ref[...].astype(F32) + got[i][l, base + s - 1, part, cut].astype(F32)).astype(BF)
                copy(l, p, s).start()
        if s == ha:
            own = rs_ref(i, l, z, part, cut)[...].astype(F32)
            g = (own + got[i][l, ha - 1, part, cut].astype(F32) + got[i][l, n - 2, part, cut].astype(F32)).astype(BF)
            out[i][l, part, cut] = g
            wide = g.astype(F32)
            mine[...] += jnp.full(mine.shape, jnp.sum(wide * wide), F32)

    def rs_drain(l, p):
        for s in range(ha):
            rs_a(l, p, s).wait_send()
        for s in range(hb):
            rs_b(l, p, s).wait_send()

    def run(ticks):
        for m, *s in ticks:
            with jax.named_scope(f"t{m}{s}"):
                rs_tick(m, *s) if len(s) == 2 else ag_tick(m, *s)

    def loop(steps, pieces, body, sched, name="loop"):
        def one(t, carry):
            for c in range(pieces):
                body(t, c)
                for (when, piece), ticks in sched.items():
                    if piece == c:
                        pl.when(t == when)(functools.partial(run, ticks))
            return carry

        with jax.named_scope(name):
            lax.fori_loop(0, steps, one, 0)

    G0, U0, D0, G1, U1, D1 = range(6)
    mine[...] = jnp.zeros_like(mine)
    get_x = pltpu.make_async_copy(x_hbm, xb, loc.at[0])
    get_dy = pltpu.make_async_copy(dy_hbm, yb, loc.at[1])
    get_x.start()
    get_dy.start()

    a = lambda m, s: (m, s)

    def rows_at(t):
        return pl.ds(pl.multiple_of(t * TILE, TILE), TILE)

    def norm0(t, c):
        rows = rows_at(t)
        wide = xb[rows, :].astype(F32)
        du[rows, pl.ds(0, d)] = (wide * scale_of(wide)).astype(BF)

    def turn(t, c):
        dt[:, rows_at(t)] = yb[rows_at(t), :].T

    run([a(G0, 0), a(U0, 0)])
    get_x.wait()
    loop(steps, 1, norm0, {}, "norm0")
    run([a(G0, 1), a(U0, 1), a(D0, 0)])
    get_dy.wait()
    loop(steps, 1, turn, {}, "turn")
    run([a(m, s + (m != D0)) for s in range(1, ha - 1) for m in (G0, U0, D0)])
    run([a(G0, 4), a(G1, 0), a(U0, 4), a(U1, 0), a(D0, 3), a(G0, 5), a(U0, 5), a(D1, 0)])
    for m in (G0, U0):
        ag_done(m)

    def cols(c):
        return pl.ds(c * CH, CH)

    def first(t, c):
        rows = rows_at(t)
        a_tile = du[rows, pl.ds(0, d)]
        gate, up = mm(a_tile, wg[0, :, cols(c)]), mm(a_tile, wu[0, :, cols(c)])
        mid[rows, cols(c)] = (gate * jax.nn.sigmoid(gate) * up).astype(BF)

    loop(steps, pieces, first, {
        (0, 0): [a(G1, 1)], (0, 1): [a(D0, 4)], (0, 2): [a(U1, 1)], (1, 0): [a(D1, 1), a(D0, 5)], (1, 2): [a(G1, 2)], (2, 0): [a(U1, 2)],
        (2, 1): [a(D1, 2)], (2, 2): [a(G1, 3)], (3, 0): [a(U1, 3)], (3, 2): [a(D1, 3)],
    }, "first")
    ag_done(D0)

    def down(t, c):
        rows = rows_at(t)
        xb[rows, :] = (xb[rows, :].astype(F32) + mm(mid[rows, :], wd[0]).astype(BF).astype(F32)).astype(BF)

    loop(steps, 1, down, {(0, 0): [a(G1, 4)], (1, 0): [a(U1, 4)], (2, 0): [a(D1, 4)], (3, 0): [a(G1, 5)]}, "down0")

    DC = ff // 4
    segments = []
    for l in (1, 0):
        segments += [(l, "prep", steps, 0.6)]
        for p in range(pieces):
            segments += [(l, f"hidden{p}", steps, 1.6), (l, f"term{p}", 2, 1.5)]
        segments += [(l, "down", ff // DC, 1.6)]
        if l:
            segments += [(l, "input", steps, 3.1)]
    agenda = plan(segments, ha, pieces)

    def hidden(l, h_ref, ct_ref):
        last = (pieces - 1) * CH

        def prep(t, _):
            rows = rows_at(t)
            wide = h_ref[rows, :].astype(F32)
            a_tile = (wide * scale_of(wide)).astype(BF)
            dg[rows, pl.ds(last, CH)] = a_tile[:, :CH]
            du[rows, pl.ds(last, d - CH)] = a_tile[:, CH:]
            at[:, rows] = a_tile.T
            if not l:
                dt[:, rows] = ct_ref[rows, :].T

        def piece(t, cut):
            rows = rows_at(t)
            a_tile = jnp.concatenate([dg[rows, pl.ds(last, CH)], du[rows, pl.ds(last, d - CH)]], axis=1)
            gate, up = mm(a_tile, wg[l, :, cut]), mm(a_tile, wu[l, :, cut])
            ct = mm_nt(ct_ref[rows, :], wd[l, cut, :]).astype(BF).astype(F32)
            s = jax.nn.sigmoid(gate)
            silu = gate * s
            mid[rows, cut] = (silu * up).astype(BF)
            du[rows, cut] = (ct * silu).astype(BF)
            dg[rows, cut] = (ct * up * (s * (1.0 + gate * (1.0 - s)))).astype(BF)

        ticks = {(t, 0): agenda[l, "prep", t] for t in range(steps) if (l, "prep", t) in agenda}
        loop(steps, 1, prep, {(1, 0): [a(U1, 5)], (3, 0): [a(D1, 5)]} if l else ticks, "prep")
        if l:
            for m in (G1, U1, D1):
                ag_done(m)

        def one_piece(p, carry):
            cut = pl.ds(pl.multiple_of(p * CH, CH), CH)

            def tile(t, carry):
                piece(t, cut)
                for q in range(pieces):
                    for when in range(steps):
                        if (l, f"hidden{q}", when) in agenda:
                            pl.when((p == q) & (t == when))(functools.partial(run, agenda[l, f"hidden{q}", when]))
                return carry

            with jax.named_scope("hidden"):
                lax.fori_loop(0, steps, tile, 0)
            with jax.named_scope("term"):
                for which, (ref, by) in enumerate(((wg, dg), (wu, du))):
                    ref[1 + l, :, cut] = mm(at[...], by[:, cut]).astype(BF)
                    for q in range(pieces):
                        if (l, f"term{q}", which) in agenda:
                            pl.when(p == q)(functools.partial(run, agenda[l, f"term{q}", which]))
            return carry

        lax.fori_loop(0, pieces, one_piece, 0)

        def term_down(c, _):
            cut = pl.ds(pl.multiple_of(c * DC, DC), DC)
            wd[1 + l, cut, :] = mm(dt[...], mid[:, cut]).astype(BF).T

        loop(ff // DC, 1, term_down, {(t, 0): agenda[l, "down", t] for t in range(ff // DC) if (l, "down", t) in agenda}, "down")

    hidden(1, xb, yb)

    def by_input(t, c):
        rows = rows_at(t)
        wide = xb[rows, :].astype(F32)
        ct = mm_nt(dg[rows, :], wg[1]).astype(BF).astype(F32) + mm_nt(du[rows, :], wu[1]).astype(BF).astype(F32)
        ct = ct.astype(BF).astype(F32)
        scale = scale_of(wide)
        inner = jnp.sum(ct * wide, -1, keepdims=True) * (scale * scale * scale) * (1.0 / d)
        by_h = (ct * scale - wide * inner).astype(BF)
        xb[rows, :] = (yb[rows, :].astype(F32) + by_h.astype(F32)).astype(BF)

    loop(steps, 1, by_input, {(t, 0): agenda[1, "input", t] for t in range(steps) if (1, "input", t) in agenda}, "input")
    get_x = pltpu.make_async_copy(x_hbm, yb, loc.at[0])
    get_x.start()
    for m in (G1, U1, D1):
        ag_drain(m)
    get_x.wait()
    hidden(0, yb, xb)
    run(agenda["after"])

    def tell(k):
        return remote(mine, theirs.at[z], all_s.at[k - 1], all_r.at[k - 1], (rep, lax.rem(z + k, n)))

    for k in range(1, n):
        tell(k).start()
    theirs[z] = mine[...]
    with jax.named_scope("drain"):
      for m in (G0, U0, D0):
        ag_drain(m)
      for l in (0, 1):
          for p in range(2 * pieces + 2):
            rs_drain(l, p)
    with jax.named_scope("tell"):
        for k in range(1, n):
            tell(k).wait()
    squares = jnp.sum(theirs[...], axis=0)[:1, :1]
    count = n * sum(s.size for s in shard)
    factor[...] = jnp.minimum(1.0, 0.5 * lax.rsqrt(squares / count + 1e-30))


def adamw(w, m, v, g):
    m = 0.9 * m + 0.1 * g
    v = 0.95 * v + 0.05 * g * g
    step = m * lax.rsqrt(v + 1e-8) + 0.1 * w
    return (w - 0.02 * step).astype(BF), m, v


def solution(mesh):
    n = mesh.shape["dp"]

    def step(x, dy, *arrays):
        weights, m, v = (arrays[i : i + 3] for i in (0, 3, 6))
        x, dy = x[0], dy[0]
        tokens, d = x.shape
        ff = weights[0].shape[2]
        ha, hb = n // 2, n - 1 - n // 2
        vmem = pl.BlockSpec(memory_space=pltpu.VMEM)
        anywhere = pl.BlockSpec(memory_space=pl.ANY)
        dma = pltpu.SemaphoreType.DMA
        flops = 17 * 2 * tokens * d * ff
        *gradients, factor = pl.pallas_call(
            functools.partial(kernel, n),
            out_shape=[jax.ShapeDtypeStruct(w.shape, BF) for w in weights] + [jax.ShapeDtypeStruct((1, 1), F32)],
            in_specs=[anywhere, anywhere, vmem, vmem, vmem],
            out_specs=[vmem] * 4,
            scratch_shapes=[
                pltpu.VMEM((3, d, ff), BF),
                pltpu.VMEM((3, d, ff), BF),
                pltpu.VMEM((3, ff, d), BF),
                *[pltpu.VMEM((2, n - 1, *w.shape[1:]), BF) for w in weights],
                *[pltpu.VMEM((tokens, ff), BF)] * 3,
                *[pltpu.VMEM((d, tokens), BF)] * 2,
                *[pltpu.VMEM((tokens, d), BF)] * 2,
                pltpu.VMEM((8, 128), F32),
                pltpu.VMEM((n, 8, 128), F32),
                dma((6, n - 1)), dma((6, n - 1)), dma((6, n - 1)), dma((6, n - 1)), dma((6, 2 * n - 2)), dma((6, 2 * n - 2)),
                dma((2 * (2 * (ff // CH) + 2), ha)), dma((2 * (2 * (ff // CH) + 2), ha)), dma((2 * (2 * (ff // CH) + 2), hb)), dma((2 * (2 * (ff // CH) + 2), hb)), dma((n - 1,)), dma((n - 1,)), dma((2,)),
            ],
            compiler_params=pltpu.CompilerParams(collective_id=0, has_side_effects=True, vmem_limit_bytes=67043328),
            cost_estimate=pl.CostEstimate(flops=flops, bytes_accessed=10 * tokens * d, transcendentals=0),
        )(x, dy, *weights)
        gradients = [g.astype(F32) * factor[0, 0] for g in gradients]
        new = [adamw(w.astype(F32), m, v, g) for w, m, v, g in zip(weights, m, v, gradients, strict=True)]
        return tuple(one[which] for which in range(3) for one in new)

    states, cut = P(("rep", "dp"), None, None), P(None, "dp", None)
    return jax.shard_map(
        step,
        mesh=mesh,
        in_specs=(states, states) + (cut,) * 9,
        out_specs=(P("rep", "dp", None),) * 9,
        check_vma=False,
    )
```

```python
import functools

import jax
import jax.numpy as jnp
from jax import lax
from jax.experimental import pallas as pl
from jax.experimental.pallas import tpu as pltpu
from jax.sharding import PartitionSpec as P

BF, F32 = jnp.bfloat16, jnp.float32
TILE = 512
CH = 512
LAG = 2
STEP = 0.2


def mm(a, b):
    return jnp.dot(a, b, preferred_element_type=F32)


def mm_nt(a, b):
    return lax.dot_general(a, b, (((1,), (1,)), ((), ())), preferred_element_type=F32)


def scale_of(wide):
    return lax.rsqrt(jnp.mean(wide * wide, -1, keepdims=True) + 1e-6)


def plan(segments, hops, pieces):
    now, free, todo, agenda = 0.0, 0.0, [], {}

    def start(tick):
        nonlocal free
        l, p, s, _ = tick
        cost = (2.63 if p >= 2 * pieces else 1.76) * (0.0 if s == hops else 0.5 if s == hops - 1 else 1.0)
        free = max(free, now) + cost
        tick[2:] = [s + 1, free + LAG]
        return (l, p, s)

    for l, kind, steps, each in segments:
        for step in range(steps):
            now += each
            if kind[:4] == "term":
                todo.append([l, step * pieces + int(kind[4:]), 0, now])
            if kind == "down" and step == steps - 1:
                todo += [[l, 2 * pieces, 0, now], [l, 2 * pieces + 1, 0, now]]
            due = sorted((t for t in todo if t[3] <= now), key=lambda t: (t[2], -t[1]))
            if due:
                agenda[l, kind, step] = [start(t) for t in due]
            todo = [t for t in todo if t[2] <= hops]
    after = []
    while todo:
        now = max(now, min(t[3] for t in todo))
        tick = min((t for t in todo if t[3] <= now), key=lambda t: (t[2], -t[1]))
        after.append(start(tick))
        now += STEP
        todo = [t for t in todo if t[2] <= hops]
    return agenda | {"after": after}


def kernel(n, x_hbm, dy_hbm, wg_in, wu_in, wd_in, og, ou, od, factor, *scratch):
    (wg, wu, wd, rg, ru, rd, mid, dg, du, at, dt, xb, yb, mine, theirs,
     agz_s, agz_r, agy_s, agy_r, agp_s, agp_r, rsa_s, rsa_r, rsb_s, rsb_r, all_s, all_r, loc) = scratch
    rep, z = lax.axis_index("rep"), lax.axis_index("dp")
    core = lax.rem(rep, 2)
    way = 1 - 2 * core
    chip = lax.rem(rep // 2, 2)
    ha = n // 2
    hb = n - 1 - ha
    tokens, d = xb.shape
    ff = mid.shape[1]

    def at_z(k):
        return lax.rem(z + way * k + n, n)

    near, far = at_z(1), at_z(-1)
    near_id, far_id, pair_id, side_id = (rep, near), (rep, far), (rep + way, z), (rep + 2 - 4 * chip, z)

    barrier = pltpu.get_barrier_semaphore()
    for k in range(1, n):
        pl.semaphore_signal(barrier, inc=1, device_id=(rep, lax.rem(z + k, n)), device_id_type=pl.DeviceIdType.MESH)
    for other in (pair_id, side_id):
        pl.semaphore_signal(barrier, inc=1, device_id=other, device_id_type=pl.DeviceIdType.MESH)
    with jax.named_scope("entry"):
        pl.semaphore_wait(barrier, n + 1)

    steps, pieces = tokens // TILE, ff // CH
    full, shard, got, out = (wg, wu, wd), (wg_in, wu_in, wd_in), (rg, ru, rd), (og, ou, od)

    def cut_of(i, ref, slot, block, first, count):
        rows, cols = shard[i].shape[1:]
        if i == 2:
            third = rows // 6
            return ref.at[slot, pl.ds(pl.multiple_of(block * rows + core * (3 * third) + first * third, 16), count * third), :]
        third = cols // 6
        return ref.at[
            slot, pl.ds(pl.multiple_of(block * rows, 16), rows), pl.ds(pl.multiple_of(core * (3 * third) + first * third, 128), count * third)
        ]

    def remote(src, dst, send, recv, to):
        return pltpu.make_async_remote_copy(
            src_ref=src, dst_ref=dst, send_sem=send, recv_sem=recv, device_id=to, device_id_type=pl.DeviceIdType.MESH
        )

    def block_of(hop):
        return at_z(-(hop + 1)) if hop < ha else at_z(hop - ha + 1)

    def ag_ring(m, hop):
        i, l = m % 3, m // 3
        s = hop if hop < ha else hop - ha
        block = at_z(-s) if hop < ha else at_z(s)
        dst = cut_of(i, full[i], l, block, chip, 2)
        src = cut_of(i, shard[i], l, 0, chip, 2) if s == 0 else dst
        return remote(src, dst, agz_s.at[m, hop], agz_r.at[m, hop], near_id if hop < ha else far_id)

    def ag_side(m, hop):
        ref = cut_of(m % 3, full[m % 3], m // 3, block_of(hop), 2 * chip, 1)
        return remote(ref, ref, agy_s.at[m, hop], agy_r.at[m, hop], side_id)

    def ag_pair(m, hop, from_side):
        first, count = (2 - 2 * chip, 1) if from_side else (chip, 2)
        ref = cut_of(m % 3, full[m % 3], m // 3, block_of(hop), first, count)
        k = from_side * (n - 1) + hop
        return remote(ref, ref, agp_s.at[m, k], agp_r.at[m, k], pair_id)

    def ag_tick(m, s):
        if s == 0:
            ag_ring(m, 0).start()
            ag_ring(m, ha).start()
            i, l = m % 3, m // 3
            rows = shard[i].shape[1]
            full[i][l, pl.ds(pl.multiple_of(z * rows, 16), rows), :] = shard[i][l]
        for base, hops in ((0, ha), (ha, hb)):
            if 1 <= s <= hops:
                hop = base + s - 1
                ag_ring(m, hop).wait_recv()
                if s < hops:
                    ag_ring(m, hop + 1).start()
                ag_side(m, hop).start()
                ag_pair(m, hop, False).start()
        for base, hops in ((0, ha), (ha, hb)):
            if 2 <= s <= hops + 1:
                hop = base + s - 2
                ag_side(m, hop).wait_recv()
                ag_pair(m, hop, True).start()

    def ag_done(m):
        with jax.named_scope(f"done{m}"):
            for hop in range(n - 1):
                ag_pair(m, hop, False).wait_recv()
                ag_pair(m, hop, True).wait_recv()

    def ag_drain(m):
        for hop in range(n - 1):
            ag_ring(m, hop).wait_send()
            ag_side(m, hop).wait_send()
            ag_pair(m, hop, False).wait_send()
            ag_pair(m, hop, True).wait_send()

    def parts_of(l, p):
        sem = l * (2 * pieces + 2) + p
        if p < 2 * pieces:
            return p // pieces, pl.ds(0, wg_in.shape[1]), pl.ds(p % pieces * CH, CH), sem
        half = wd_in.shape[1] // 2
        return 2, pl.ds((p - 2 * pieces) * half, half), slice(None), sem

    def rs_ref(i, l, block, part, cut):
        return full[i].at[1 + l, pl.ds(pl.multiple_of(block * shard[i].shape[1] + part.start, 16), part.size), cut]

    def rs_a(l, p, s):
        i, part, cut, sem = parts_of(l, p)
        return remote(rs_ref(i, l, at_z(ha - s), part, cut), got[i].at[l, s, part, cut], rsa_s.at[sem, s], rsa_r.at[sem, s], near_id)

    def rs_b(l, p, s):
        i, part, cut, sem = parts_of(l, p)
        return remote(
            rs_ref(i, l, at_z(-(hb - s)), part, cut), got[i].at[l, ha + s, part, cut], rsb_s.at[sem, s], rsb_r.at[sem, s], far_id
        )

    def rs_tick(l, p, s):
        i, part, cut, _ = parts_of(l, p)
        for copy, hops, base, sense in ((rs_a, ha, 0, 1), (rs_b, hb, ha, -1)):
            if s and s <= hops:
                copy(l, p, s - 1).wait_recv()
            if s < hops:
                if s:
                    ref = rs_ref(i, l, at_z(sense * (hops - s)), part, cut)
                    ref[...] = (ref[...].astype(F32) + got[i][l, base + s - 1, part, cut].astype(F32)).astype(BF)
                copy(l, p, s).start()
        if s == ha:
            own = rs_ref(i, l, z, part, cut)[...].astype(F32)
            g = (own + got[i][l, ha - 1, part, cut].astype(F32) + got[i][l, n - 2, part, cut].astype(F32)).astype(BF)
            out[i][l, part, cut] = g
            wide = g.astype(F32)
            mine[...] += jnp.full(mine.shape, jnp.sum(wide * wide), F32)

    def rs_drain(l, p):
        for s in range(ha):
            rs_a(l, p, s).wait_send()
        for s in range(hb):
            rs_b(l, p, s).wait_send()

    def run(ticks):
        for m, *s in ticks:
            with jax.named_scope(f"t{m}{s}"):
                rs_tick(m, *s) if len(s) == 2 else ag_tick(m, *s)

    def loop(steps, pieces, body, sched, name="loop"):
        def one(t, carry):
            for c in range(pieces):
                body(t, c)
                for (when, piece), ticks in sched.items():
                    if piece == c:
                        pl.when(t == when)(functools.partial(run, ticks))
            return carry

        with jax.named_scope(name):
            lax.fori_loop(0, steps, one, 0)

    G0, U0, D0, G1, U1, D1 = range(6)
    mine[...] = jnp.zeros_like(mine)
    get_x = pltpu.make_async_copy(x_hbm, xb, loc.at[0])
    get_dy = pltpu.make_async_copy(dy_hbm, yb, loc.at[1])
    get_x.start()
    get_dy.start()

    a = lambda m, s: (m, s)

    def rows_at(t):
        return pl.ds(pl.multiple_of(t * TILE, TILE), TILE)

    def norm0(t, c):
        rows = rows_at(t)
        wide = xb[rows, :].astype(F32)
        du[rows, pl.ds(0, d)] = (wide * scale_of(wide)).astype(BF)

    def turn(t, c):
        dt[:, rows_at(t)] = yb[rows_at(t), :].T

    run([a(G0, 0), a(U0, 0)])
    get_x.wait()
    loop(steps, 1, norm0, {}, "norm0")
    run([a(G0, 1), a(U0, 1), a(D0, 0)])
    get_dy.wait()
    loop(steps, 1, turn, {}, "turn")
    run([a(m, s + (m != D0)) for s in range(1, ha - 1) for m in (G0, U0, D0)])
    run([a(G0, 4), a(G1, 0), a(U0, 4), a(U1, 0), a(D0, 3), a(G0, 5), a(U0, 5), a(D1, 0)])
    for m in (G0, U0):
        ag_done(m)

    def cols(c):
        return pl.ds(c * CH, CH)

    def first(t, c):
        rows = rows_at(t)
        a_tile = du[rows, pl.ds(0, d)]
        gate, up = mm(a_tile, wg[0, :, cols(c)]), mm(a_tile, wu[0, :, cols(c)])
        mid[rows, cols(c)] = (gate * jax.nn.sigmoid(gate) * up).astype(BF)

    loop(steps, pieces, first, {
        (0, 0): [a(G1, 1)], (0, 1): [a(D0, 4)], (0, 2): [a(U1, 1)], (1, 0): [a(D1, 1), a(D0, 5)], (1, 2): [a(G1, 2)], (2, 0): [a(U1, 2)],
        (2, 1): [a(D1, 2)], (2, 2): [a(G1, 3)], (3, 0): [a(U1, 3)], (3, 2): [a(D1, 3)],
    }, "first")
    ag_done(D0)

    def down(t, c):
        rows = rows_at(t)
        xb[rows, :] = (xb[rows, :].astype(F32) + mm(mid[rows, :], wd[0]).astype(BF).astype(F32)).astype(BF)

    loop(steps, 1, down, {(0, 0): [a(G1, 4)], (1, 0): [a(U1, 4)], (2, 0): [a(D1, 4)], (3, 0): [a(G1, 5)]}, "down0")

    DC = ff // 4
    segments = []
    for l in (1, 0):
        segments += [(l, "prep", steps, 0.6)]
        for p in range(pieces):
            segments += [(l, f"hidden{p}", steps, 1.6), (l, f"term{p}", 2, 1.5)]
        segments += [(l, "down", ff // DC, 1.6)]
        if l:
            segments += [(l, "input", steps, 3.1)]
    agenda = plan(segments, ha, pieces)

    def hidden(l, h_ref, ct_ref):
        last = (pieces - 1) * CH

        def prep(t, _):
            rows = rows_at(t)
            wide = h_ref[rows, :].astype(F32)
            a_tile = (wide * scale_of(wide)).astype(BF)
            dg[rows, pl.ds(last, CH)] = a_tile[:, :CH]
            du[rows, pl.ds(last, d - CH)] = a_tile[:, CH:]
            at[:, rows] = a_tile.T
            if not l:
                dt[:, rows] = ct_ref[rows, :].T

        def piece(t, cut):
            rows = rows_at(t)
            a_tile = jnp.concatenate([dg[rows, pl.ds(last, CH)], du[rows, pl.ds(last, d - CH)]], axis=1)
            gate, up = mm(a_tile, wg[l, :, cut]), mm(a_tile, wu[l, :, cut])
            ct = mm_nt(ct_ref[rows, :], wd[l, cut, :]).astype(BF).astype(F32)
            s = jax.nn.sigmoid(gate)
            silu = gate * s
            mid[rows, cut] = (silu * up).astype(BF)
            du[rows, cut] = (ct * silu).astype(BF)
            dg[rows, cut] = (ct * up * (s * (1.0 + gate * (1.0 - s)))).astype(BF)

        ticks = {(t, 0): agenda[l, "prep", t] for t in range(steps) if (l, "prep", t) in agenda}
        loop(steps, 1, prep, {(1, 0): [a(U1, 5)], (3, 0): [a(D1, 5)]} if l else ticks, "prep")
        if l:
            for m in (G1, U1, D1):
                ag_done(m)

        def one_piece(p, carry):
            cut = pl.ds(pl.multiple_of(p * CH, CH), CH)

            def tile(t, carry):
                piece(t, cut)
                for q in range(pieces):
                    for when in range(steps):
                        if (l, f"hidden{q}", when) in agenda:
                            pl.when((p == q) & (t == when))(functools.partial(run, agenda[l, f"hidden{q}", when]))
                return carry

            with jax.named_scope("hidden"):
                lax.fori_loop(0, steps, tile, 0)
            with jax.named_scope("term"):
                for which, (ref, by) in enumerate(((wg, dg), (wu, du))):
                    ref[1 + l, :, cut] = mm(at[...], by[:, cut]).astype(BF)
                    for q in range(pieces):
                        if (l, f"term{q}", which) in agenda:
                            pl.when(p == q)(functools.partial(run, agenda[l, f"term{q}", which]))
            return carry

        lax.fori_loop(0, pieces, one_piece, 0)

        def term_down(c, _):
            cut = pl.ds(pl.multiple_of(c * DC, DC), DC)
            wd[1 + l, cut, :] = mm(dt[...], mid[:, cut]).astype(BF).T

        loop(ff // DC, 1, term_down, {(t, 0): agenda[l, "down", t] for t in range(ff // DC) if (l, "down", t) in agenda}, "down")

    hidden(1, xb, yb)

    def by_input(t, c):
        rows = rows_at(t)
        wide = xb[rows, :].astype(F32)
        ct = mm_nt(dg[rows, :], wg[1]).astype(BF).astype(F32) + mm_nt(du[rows, :], wu[1]).astype(BF).astype(F32)
        ct = ct.astype(BF).astype(F32)
        scale = scale_of(wide)
        inner = jnp.sum(ct * wide, -1, keepdims=True) * (scale * scale * scale) * (1.0 / d)
        by_h = (ct * scale - wide * inner).astype(BF)
        xb[rows, :] = (yb[rows, :].astype(F32) + by_h.astype(F32)).astype(BF)

    loop(steps, 1, by_input, {(t, 0): agenda[1, "input", t] for t in range(steps) if (1, "input", t) in agenda}, "input")
    get_x = pltpu.make_async_copy(x_hbm, yb, loc.at[0])
    get_x.start()
    for m in (G1, U1, D1):
        ag_drain(m)
    get_x.wait()
    hidden(0, yb, xb)
    run(agenda["after"])

    def tell(k):
        return remote(mine, theirs.at[z], all_s.at[k - 1], all_r.at[k - 1], (rep, lax.rem(z + k, n)))

    for k in range(1, n):
        tell(k).start()
    theirs[z] = mine[...]
    with jax.named_scope("drain"):
      for m in (G0, U0, D0):
        ag_drain(m)
      for l in (0, 1):
          for p in range(2 * pieces + 2):
            rs_drain(l, p)
    with jax.named_scope("tell"):
        for k in range(1, n):
            tell(k).wait()
    squares = jnp.sum(theirs[...], axis=0)[:1, :1]
    count = n * sum(s.size for s in shard)
    factor[...] = jnp.minimum(1.0, 0.5 * lax.rsqrt(squares / count + 1e-30))


def adamw(w, m, v, g):
    m = 0.9 * m + 0.1 * g
    v = 0.95 * v + 0.05 * g * g
    step = m * lax.rsqrt(v + 1e-8) + 0.1 * w
    return (w - 0.02 * step).astype(BF), m, v


def update(factor, *refs):
    for i in range(3):
        w, m, v, g, new_w, new_m, new_v = (refs[3 * k + i] for k in range(7))
        new_w[...], new_m[...], new_v[...] = adamw(w[...].astype(F32), m[...], v[...], g[...].astype(F32) * factor[...].reshape(1, 1, 1))


def solution(mesh):
    n = mesh.shape["dp"]

    def step(x, dy, *arrays):
        weights, m, v = (arrays[i : i + 3] for i in (0, 3, 6))
        x, dy = x[0], dy[0]
        tokens, d = x.shape
        ff = weights[0].shape[2]
        ha, hb = n // 2, n - 1 - n // 2
        vmem = pl.BlockSpec(memory_space=pltpu.VMEM)
        anywhere = pl.BlockSpec(memory_space=pl.ANY)
        dma = pltpu.SemaphoreType.DMA
        flops = 17 * 2 * tokens * d * ff
        *gradients, factor = pl.pallas_call(
            functools.partial(kernel, n),
            out_shape=[jax.ShapeDtypeStruct(w.shape, BF) for w in weights] + [jax.ShapeDtypeStruct((1, 1), F32)],
            in_specs=[anywhere, anywhere, vmem, vmem, vmem],
            out_specs=[vmem] * 4,
            scratch_shapes=[
                pltpu.VMEM((3, d, ff), BF),
                pltpu.VMEM((3, d, ff), BF),
                pltpu.VMEM((3, ff, d), BF),
                *[pltpu.VMEM((2, n - 1, *w.shape[1:]), BF) for w in weights],
                *[pltpu.VMEM((tokens, ff), BF)] * 3,
                *[pltpu.VMEM((d, tokens), BF)] * 2,
                *[pltpu.VMEM((tokens, d), BF)] * 2,
                pltpu.VMEM((8, 128), F32),
                pltpu.VMEM((n, 8, 128), F32),
                dma((6, n - 1)), dma((6, n - 1)), dma((6, n - 1)), dma((6, n - 1)), dma((6, 2 * n - 2)), dma((6, 2 * n - 2)),
                dma((2 * (2 * (ff // CH) + 2), ha)), dma((2 * (2 * (ff // CH) + 2), ha)), dma((2 * (2 * (ff // CH) + 2), hb)), dma((2 * (2 * (ff // CH) + 2), hb)), dma((n - 1,)), dma((n - 1,)), dma((2,)),
            ],
            compiler_params=pltpu.CompilerParams(collective_id=0, has_side_effects=True, vmem_limit_bytes=67043328),
            cost_estimate=pl.CostEstimate(flops=flops, bytes_accessed=10 * tokens * d, transcendentals=0),
        )(x, dy, *weights)
        blocks = [pl.BlockSpec((1, w.shape[1] // 2, w.shape[2]), lambda l, i: (l, i, 0)) for w in weights]
        return tuple(
            pl.pallas_call(
                update,
                grid=(weights[0].shape[0], 2),
                out_shape=[jax.ShapeDtypeStruct(w.shape, dtype) for dtype in (BF, F32, F32) for w in weights],
                in_specs=[pl.BlockSpec((1, 1), lambda l, i: (0, 0)), *blocks * 4],
                out_specs=blocks * 3,
            )(factor, *weights, *m, *v, *gradients)
        )

    states, cut = P(("rep", "dp"), None, None), P(None, "dp", None)
    return jax.shard_map(
        step,
        mesh=mesh,
        in_specs=(states, states) + (cut,) * 9,
        out_specs=(P("rep", "dp", None),) * 9,
        check_vma=False,
    )
```
